32 devices in a mesh: py: 2 (over x), px: 4 (over z), pz: 4 (over y, core).
Axes of the slice: x: 2, y: 2, z: 4, core: 2. Of those that a mesh axis runs over, the one named last changes fastest.
Arguments:
- field_now: float32 [16, 64, 256, 128], P('py', 'px', 'pz'), may hold values from 0.2 to 1.8
- earlier: float32 [16, 64, 256, 128], P('py', 'px', 'pz'), may hold values from 0.2 to 1.8
- speed_square: float32 [16, 64, 256, 128], P('py', 'px', 'pz'), may hold values from 0.05 to 0.3
Outputs:
- column_sum: float32 [16, 64, 256, 128], P('py', 'px', 'pz')
- field_now_end: float32 [16, 64, 256, 128], P('py', 'px', 'pz')
The draws below stay inside these ranges and needn't reach their ends.
All inputs are finite; a program needn't handle non-finite values.
Results may differ from the reference program's by a relative error of at most 0.00002.
Values sent between devices are 32-bit elements; how exact they have to be, the bound alone decides.
A program may use at most 128 MiB of HBM per device.

```python
import jax
import jax.numpy as jnp
from jax import lax

GRID_J = 16
GRID_I = 64
GRID_K = 256
LEVELS = 128
STEPS = 4


def shard_levels(key, extent, split, low, top_value):
    level = 1.0
    for position, shards_of in split:
        heights = jax.random.uniform(jax.random.fold_in(jax.random.fold_in(key, 6), position), (shards_of,), jnp.float32, low / len(split), top_value / len(split))
        level = level * jnp.repeat(jnp.exp(heights), extent[position] // shards_of).reshape((-1,) + (1,) * (len(extent) - 1 - position))
    return level


def setup_inputs(seed: int = 0) -> dict:
    seeds = jax.random.split(jax.random.key(seed), 4)
    field_now = jnp.clip(0.2 + 1.5999999 * jax.random.uniform(seeds[0], (GRID_J, GRID_I, GRID_K, LEVELS), jnp.float32) ** shard_levels(seeds[0], (GRID_J, GRID_I, GRID_K, LEVELS), ((0, 2), (1, 4), (2, 4)), -0.2, 0.2), 0.2, 1.8)
    earlier = jnp.clip(0.2 + 1.5999999 * jax.random.uniform(seeds[1], (GRID_J, GRID_I, GRID_K, LEVELS), jnp.float32) ** shard_levels(seeds[1], (GRID_J, GRID_I, GRID_K, LEVELS), ((0, 2), (1, 4), (2, 4)), -0.2, 0.2), 0.2, 1.8)
    speed_square = jnp.clip(0.05 + 0.25 * jax.random.uniform(seeds[2], (GRID_J, GRID_I, GRID_K, LEVELS), jnp.float32) ** shard_levels(seeds[2], (GRID_J, GRID_I, GRID_K, LEVELS), ((0, 2), (1, 4), (2, 4)), -0.2, 0.2), 0.05, 0.3)
    return dict(field_now=field_now, earlier=earlier, speed_square=speed_square)


def without_rim(values, dims):
    for dim in dims:
        values = lax.slice_in_dim(values, 1, values.shape[dim] - 1, axis=dim)
    return values


def shifted_cells(values, dim, start, dims):
    others = [other for other in dims if other != dim]
    values = without_rim(values, others)
    return lax.slice_in_dim(values, start, start + values.shape[dim] - 2, axis=dim)


def march_step(padded, before, speed_square):
    middle = without_rim(padded, (0, 1, 2))
    lower = [shifted_cells(padded, dim, 0, (0, 1, 2)) for dim in (0, 1, 2)]
    upper = [shifted_cells(padded, dim, 2, (0, 1, 2)) for dim in (0, 1, 2)]
    spread = lower[0] + upper[0] + lower[1] + upper[1] + lower[2] + upper[2] - 6.0 * middle
    return 2.0 * middle - before + speed_square * spread


def reference(field_now, earlier, speed_square):
    for step in range(STEPS):
        later = march_step(jnp.pad(field_now, ((1, 1), (1, 1), (1, 1), (0, 0)), mode="wrap"), earlier, speed_square)
        earlier, field_now = field_now, later
    column_sum = jnp.cumsum(field_now, axis=0) / GRID_J
    return column_sum, field_now
```

```python
import functools

import jax
import jax.numpy as jnp
from jax import lax
from jax.experimental import pallas as pl
from jax.experimental.pallas import tpu as pltpu
from jax.sharding import PartitionSpec as P

STEPS = 4
CHUNKS = 4
MESH = pl.DeviceIdType.MESH


def march_kernel(
    peers, chunks, field, before, speed, sums_out, field_out,
    u, cs, csum, total, acc, below, ysend, yrecv,
    load_sem, x_send, x_recv, z_send, z_recv, y_send, y_recv, t_send, t_recv, out_sem, sum_sem,
):
    J, I, K, L = field.shape
    ny, nx, nz = peers
    width = I // chunks
    my, mx, mz = (lax.axis_index(a) for a in ("py", "px", "pz"))
    y_side = ({"py": lax.rem(my + 1, ny)}, {"py": lax.rem(my + ny - 1, ny)})
    x_side = ({"px": lax.rem(mx + 1, nx)}, {"px": lax.rem(mx + nx - 1, nx)})
    z_side = ({"pz": lax.rem(mz + 1, nz)}, {"pz": lax.rem(mz + nz - 1, nz)})
    parts = ((1, J - 2), (0, 1), (J - 1, 1))

    loads = [
        pltpu.make_async_copy(field, u.at[0, pl.ds(1, J), pl.ds(1, I)], load_sem.at[0]),
        pltpu.make_async_copy(before, u.at[1, pl.ds(1, J), pl.ds(1, I)], load_sem.at[1]),
        pltpu.make_async_copy(speed, cs, load_sem.at[2]),
    ]
    for load in loads:
        load.start()

    barrier = pltpu.get_barrier_semaphore()
    for d in range(1, ny):
        pl.semaphore_signal(barrier, inc=1, device_id={"py": lax.rem(my + d, ny)}, device_id_type=MESH)
    for side in x_side + z_side:
        pl.semaphore_signal(barrier, inc=1, device_id=side, device_id_type=MESH)
    pl.semaphore_wait(barrier, ny - 1 + 4)

    def remote(src, dst, send, recv, to):
        return pltpu.make_async_remote_copy(
            src_ref=src, dst_ref=dst, send_sem=send, recv_sem=recv, device_id=to, device_id_type=MESH
        )

    def j_copy(t, side, c):
        row, rim = ((J - 1, 0), (0, J + 1))[side]
        here = pl.ds(c * width, width)
        there = pl.ds(1 + c * width, width)
        src = field.at[row, here] if t == 0 else u.at[t % 2, row + 1, there]
        return remote(src, u.at[t % 2, rim, there], x_send.at[t, side, c], x_recv.at[t, side, c], y_side[side])

    def i_copy(t, side, part):
        plane, rim = ((I - 1, 0), (0, I + 1))[side]
        start, size = parts[part]
        rows = pl.ds(start + 1, size)
        src = field.at[pl.ds(start, size), plane] if t == 0 else u.at[t % 2, rows, plane + 1]
        return remote(src, u.at[t % 2, rows, rim], z_send.at[t, side, part], z_recv.at[t, side, part], x_side[side])

    def k_copy(t, side, part):
        start, size = parts[part]
        rows = pl.ds(start, size)
        return remote(
            ysend.at[t, side, rows], yrecv.at[t, side, rows],
            y_send.at[t, side, part], y_recv.at[t, side, part], z_side[side],
        )

    def pack(t, j, i, value):
        ysend[t, 0, j, pl.ds(i, 1), :] = value[K - 1:K]
        ysend[t, 1, j, pl.ds(i, 1), :] = value[0:1]

    for c in range(chunks):
        for side in (0, 1):
            j_copy(0, side, c).start()
    for part in range(3):
        for side in (0, 1):
            i_copy(0, side, part).start()

    loads[0].wait()

    def pack_row(j, carry):
        for i in range(I):
            ysend[0, 0, j, i:i + 1, :] = u[0, j + 1, i + 1, K - 1:K, :]
            ysend[0, 1, j, i:i + 1, :] = u[0, j + 1, i + 1, 0:1, :]
        return carry

    lax.fori_loop(0, J, pack_row, 0)
    for part in range(3):
        for side in (0, 1):
            k_copy(0, side, part).start()
    loads[1].wait()
    loads[2].wait()

    k_index = lax.broadcasted_iota(jnp.int32, (K, L), 0)

    def column(t, j, i):
        now, other = t % 2, (t + 1) % 2
        middle = u[now, j + 1, i + 1]
        low = jnp.where(k_index == 0, yrecv[t, 0, j, pl.ds(i, 1), :], pltpu.roll(middle, 1, 0))
        high = jnp.where(k_index == K - 1, yrecv[t, 1, j, pl.ds(i, 1), :], pltpu.roll(middle, K - 1, 0))
        spread = (
            u[now, j, i + 1] + u[now, j + 2, i + 1] + u[now, j + 1, i] + u[now, j + 1, i + 2]
            + low + high - 6.0 * middle
        )
        later = 2.0 * middle - u[other, j + 1, i + 1] + cs[j, i] * spread
        u[other, j + 1, i + 1] = later
        if t + 1 < STEPS:
            pack(t + 1, j, i, later)

    def out_copy(part, c):
        start, size = parts[part]
        here = pl.ds(0, I) if part == 0 else pl.ds(c * width, width)
        there = pl.ds(1, I) if part == 0 else pl.ds(1 + c * width, width)
        rows = pl.ds(start, size)
        return pltpu.make_async_copy(
            u.at[STEPS % 2, pl.ds(start + 1, size), there], field_out.at[rows, here], out_sem.at[part, c]
        )

    def total_copy(d, c):
        here = pl.ds(c * width, width)
        return remote(
            total.at[here], below.at[d - 1, here], t_send.at[d - 1, c], t_recv.at[d - 1, c],
            {"py": lax.rem(my + d, ny)},
        )

    for t in range(STEPS):
        last = t + 1 == STEPS
        for side in (0, 1):
            i_copy(t, side, 0).wait_recv()
            k_copy(t, side, 0).wait_recv()
            if t > 0:
                i_copy(t - 1, side, 0).wait_send()

        def inner(q, carry, t=t):
            j = 1 + q // (I // 2)
            i = lax.rem(q, I // 2) * 2
            column(t, j, i)
            column(t, j, i + 1)
            return carry

        lax.fori_loop(0, (J - 2) * (I // 2), inner, 0)
        if not last:
            for side in (0, 1):
                i_copy(t + 1, side, 0).start()
                k_copy(t + 1, side, 0).start()
        else:
            out_copy(0, 0).start()

        for side in (0, 1):
            for part in (1, 2):
                i_copy(t, side, part).wait_recv()
                k_copy(t, side, part).wait_recv()
                if t > 0:
                    i_copy(t - 1, side, part).wait_send()
        for c in range(chunks):
            for side in (0, 1):
                j_copy(t, side, c).wait_recv()
                if t > 0:
                    j_copy(t - 1, side, c).wait_send()

            def outer(q, carry, t=t, c=c):
                i = c * width + q
                column(t, 0, i)
                column(t, J - 1, i)
                return carry

            lax.fori_loop(0, width, outer, 0)
            if not last:
                for side in (0, 1):
                    j_copy(t + 1, side, c).start()
            else:
                def add_up(q, carry, c=c):
                    i = c * width + q
                    value = u[STEPS % 2, 1, i + 1]
                    for j in range(1, J):
                        value = value + u[STEPS % 2, j + 1, i + 1]
                    total[i] = value
                    return carry

                lax.fori_loop(0, width, add_up, 0)
                for d in range(1, ny):
                    @pl.when(my + d < ny)
                    def _(d=d, c=c):
                        total_copy(d, c).start()
                for part in (1, 2):
                    out_copy(part, c).start()
        if not last:
            for part in (1, 2):
                for side in (0, 1):
                    i_copy(t + 1, side, part).start()
                    k_copy(t + 1, side, part).start()

    scale = 1.0 / (J * ny)

    def sum_copy(c):
        here = pl.ds(c * width, width)
        return pltpu.make_async_copy(csum.at[:, here], sums_out.at[:, here], sum_sem.at[c])

    for c in range(chunks):
        here = pl.ds(c * width, width)
        acc[...] = jnp.zeros_like(acc)
        for d in range(1, ny):
            @pl.when(my >= d)
            def _(d=d, c=c, here=here):
                total_copy(d, c).wait_recv()
                acc[...] = acc[...] + below[d - 1, here]

        def running(q, carry, c=c):
            i = c * width + q
            value = acc[q]
            for j in range(J):
                value = value + u[STEPS % 2, j + 1, i + 1]
                csum[j, i] = value * scale
            return carry

        lax.fori_loop(0, width, running, 0)
        sum_copy(c).start()

    for side in (0, 1):
        for c in range(chunks):
            j_copy(STEPS - 1, side, c).wait_send()
        for part in range(3):
            i_copy(STEPS - 1, side, part).wait_send()
            for t in range(STEPS):
                k_copy(t, side, part).wait_send()
    for c in range(chunks):
        for d in range(1, ny):
            @pl.when(my + d < ny)
            def _(d=d, c=c):
                total_copy(d, c).wait_send()
        for part in (1, 2):
            out_copy(part, c).wait()
        sum_copy(c).wait()
    out_copy(0, 0).wait()


def local(peers, field_now, earlier, speed_square):
    J, I, K, L = field_now.shape
    chunks = CHUNKS if I % CHUNKS == 0 else 1
    ny = peers[0]
    f32 = jnp.float32
    dma = pltpu.SemaphoreType.DMA
    anywhere = pl.BlockSpec(memory_space=pltpu.MemorySpace.HBM)
    shape = jax.ShapeDtypeStruct(field_now.shape, f32)
    slots = max(ny - 1, 1)
    return pl.pallas_call(
        functools.partial(march_kernel, peers, chunks),
        out_shape=(shape, shape),
        in_specs=[anywhere] * 3,
        out_specs=(anywhere, anywhere),
        scratch_shapes=[
            pltpu.VMEM((2, J + 2, I + 2, K, L), f32),
            pltpu.VMEM((J, I, K, L), f32),
            pltpu.VMEM((J, I, K, L), f32),
            pltpu.VMEM((I, K, L), f32),
            pltpu.VMEM((I // chunks, K, L), f32),
            pltpu.VMEM((slots, I, K, L), f32),
            pltpu.VMEM((STEPS, 2, J, I, L), f32),
            pltpu.VMEM((STEPS, 2, J, I, L), f32),
            dma((3,)),
            dma((STEPS, 2, chunks)),
            dma((STEPS, 2, chunks)),
            dma((STEPS, 2, 3)),
            dma((STEPS, 2, 3)),
            dma((STEPS, 2, 3)),
            dma((STEPS, 2, 3)),
            dma((slots, chunks)),
            dma((slots, chunks)),
            dma((3, chunks)),
            dma((chunks,)),
        ],
        compiler_params=pltpu.CompilerParams(
            collective_id=0, has_side_effects=True, vmem_limit_bytes=60 * 1024 * 1024
        ),
        name="march",
    )(field_now, earlier, speed_square)


def solution(mesh):
    placed = P("py", "px", "pz", None)
    peers = tuple(mesh.shape[a] for a in ("py", "px", "pz"))
    return jax.shard_map(
        functools.partial(local, peers),
        mesh=mesh,
        in_specs=(placed,) * 3,
        out_specs=(placed,) * 2,
        check_vma=False,
    )
```

```python
import functools

import jax
import jax.numpy as jnp
from jax import lax
from jax.experimental import pallas as pl
from jax.experimental.pallas import tpu as pltpu
from jax.sharding import PartitionSpec as P

STEPS = 4
CHUNKS = 4
MESH = pl.DeviceIdType.MESH


def march_kernel(
    peers, chunks, field, before, speed, end, under,
    u, cs, total, below, ysend, yrecv,
    load_sem, x_send, x_recv, z_send, z_recv, y_send, y_recv, t_send, t_recv,
):
    J, I, K, L = field.shape
    ny, nx, nz = peers
    width = I // chunks
    my, mx, mz = (lax.axis_index(a) for a in ("py", "px", "pz"))
    y_side = ({"py": lax.rem(my + 1, ny)}, {"py": lax.rem(my + ny - 1, ny)})
    x_side = ({"px": lax.rem(mx + 1, nx)}, {"px": lax.rem(mx + nx - 1, nx)})
    z_side = ({"pz": lax.rem(mz + 1, nz)}, {"pz": lax.rem(mz + nz - 1, nz)})
    parts = ((1, J - 2), (0, 1), (J - 1, 1))

    loads = [
        pltpu.make_async_copy(
            field.at[pl.ds(start, size)], u.at[0, pl.ds(start + 1, size), pl.ds(1, I)], load_sem.at[part]
        )
        for part, (start, size) in reversed(tuple(enumerate(parts)))
    ] + [
        pltpu.make_async_copy(before, u.at[1, pl.ds(1, J), pl.ds(1, I)], load_sem.at[3]),
        pltpu.make_async_copy(speed, cs, load_sem.at[4]),
    ]
    for load in loads:
        load.start()

    barrier = pltpu.get_barrier_semaphore()
    for d in range(1, ny):
        pl.semaphore_signal(barrier, inc=1, device_id={"py": lax.rem(my + d, ny)}, device_id_type=MESH)
    for side in x_side + z_side:
        pl.semaphore_signal(barrier, inc=1, device_id=side, device_id_type=MESH)
    pl.semaphore_wait(barrier, ny - 1 + 4)

    def remote(src, dst, send, recv, to):
        return pltpu.make_async_remote_copy(
            src_ref=src, dst_ref=dst, send_sem=send, recv_sem=recv, device_id=to, device_id_type=MESH
        )

    def j_copy(t, side, c):
        row, rim = ((J - 1, 0), (0, J + 1))[side]
        there = pl.ds(1 + c * width, width)
        return remote(u.at[t % 2, row + 1, there], u.at[t % 2, rim, there], x_send.at[t, side, c], x_recv.at[t, side, c], y_side[side])

    def i_copy(t, side, part):
        plane, rim = ((I - 1, 0), (0, I + 1))[side]
        start, size = parts[part]
        rows = pl.ds(start + 1, size)
        src = field.at[pl.ds(start, size), plane] if t == 0 else u.at[t % 2, rows, plane + 1]
        return remote(src, u.at[t % 2, rows, rim], z_send.at[t, side, part], z_recv.at[t, side, part], x_side[side])

    def k_copy(t, side, part):
        start, size = parts[part]
        rows = pl.ds(start, size)
        return remote(
            ysend.at[t, side, rows], yrecv.at[t, side, rows],
            y_send.at[t, side, part], y_recv.at[t, side, part], z_side[side],
        )

    def pack(t, j, i, value):
        ysend[t, 0, j, pl.ds(i, 1), :] = value[K - 1:K]
        ysend[t, 1, j, pl.ds(i, 1), :] = value[0:1]

    for side in (0, 1):
        loads[side].wait()
    for c in range(chunks):
        for side in (0, 1):
            j_copy(0, side, c).start()
    for part in range(3):
        for side in (0, 1):
            i_copy(0, side, part).start()

    loads[2].wait()

    def pack_row(j, carry):
        for i in range(I):
            ysend[0, 0, j, i:i + 1, :] = u[0, j + 1, i + 1, K - 1:K, :]
            ysend[0, 1, j, i:i + 1, :] = u[0, j + 1, i + 1, 0:1, :]
        return carry

    lax.fori_loop(0, J, pack_row, 0)
    for part in range(3):
        for side in (0, 1):
            k_copy(0, side, part).start()
    loads[3].wait()
    loads[4].wait()

    k_index = lax.broadcasted_iota(jnp.int32, (K, L), 0)

    def column(t, j, i):
        now, other = t % 2, (t + 1) % 2
        middle = u[now, j + 1, i + 1]
        low = jnp.where(k_index == 0, yrecv[t, 0, j, pl.ds(i, 1), :], pltpu.roll(middle, 1, 0))
        high = jnp.where(k_index == K - 1, yrecv[t, 1, j, pl.ds(i, 1), :], pltpu.roll(middle, K - 1, 0))
        spread = (
            u[now, j, i + 1] + u[now, j + 2, i + 1] + u[now, j + 1, i] + u[now, j + 1, i + 2]
            + low + high - 6.0 * middle
        )
        later = 2.0 * middle - u[other, j + 1, i + 1] + cs[j, i] * spread
        if t + 1 < STEPS:
            u[other, j + 1, i + 1] = later
            pack(t + 1, j, i, later)
        else:
            end[j, i] = later

    def total_copy(d, c):
        here = pl.ds(c * width, width)
        return remote(
            total.at[here], below.at[d - 1, here], t_send.at[d - 1, c], t_recv.at[d - 1, c],
            {"py": lax.rem(my + d, ny)},
        )

    for t in range(STEPS):
        last = t + 1 == STEPS
        for side in (0, 1):
            i_copy(t, side, 0).wait_recv()
            k_copy(t, side, 0).wait_recv()
            if t > 0:
                i_copy(t - 1, side, 0).wait_send()

        def inner(q, carry, t=t):
            j = 1 + q // (I // 2)
            i = lax.rem(q, I // 2) * 2
            column(t, j, i)
            column(t, j, i + 1)
            return carry

        lax.fori_loop(0, (J - 2) * (I // 2), inner, 0)
        if not last:
            for side in (0, 1):
                i_copy(t + 1, side, 0).start()
                k_copy(t + 1, side, 0).start()

        for side in (0, 1):
            for part in (1, 2):
                i_copy(t, side, part).wait_recv()
                k_copy(t, side, part).wait_recv()
                if t > 0:
                    i_copy(t - 1, side, part).wait_send()
        for c in range(chunks):
            for side in (0, 1):
                j_copy(t, side, c).wait_recv()
                if t > 0:
                    j_copy(t - 1, side, c).wait_send()

            def outer(q, carry, t=t, c=c):
                i = c * width + q
                column(t, 0, i)
                column(t, J - 1, i)
                return carry

            lax.fori_loop(0, width, outer, 0)
            if not last:
                for side in (0, 1):
                    j_copy(t + 1, side, c).start()
            else:
                def add_up(q, carry, c=c):
                    i = c * width + q
                    value = end[0, i]
                    for j in range(1, J):
                        value = value + end[j, i]
                    total[i] = value
                    return carry

                lax.fori_loop(0, width, add_up, 0)
                for d in range(1, ny):
                    @pl.when(my + d < ny)
                    def _(d=d, c=c):
                        total_copy(d, c).start()
        if not last:
            for part in (1, 2):
                for side in (0, 1):
                    i_copy(t + 1, side, part).start()
                    k_copy(t + 1, side, part).start()

    for c in range(chunks):
        here = pl.ds(c * width, width)
        under[here] = jnp.zeros((width, K, L), jnp.float32)
        for d in range(1, ny):
            @pl.when(my >= d)
            def _(d=d, c=c, here=here):
                total_copy(d, c).wait_recv()
                under[here] = under[here] + below[d - 1, here]

    for side in (0, 1):
        for c in range(chunks):
            j_copy(STEPS - 1, side, c).wait_send()
        for part in range(3):
            i_copy(STEPS - 1, side, part).wait_send()
            for t in range(STEPS):
                k_copy(t, side, part).wait_send()
    for c in range(chunks):
        for d in range(1, ny):
            @pl.when(my + d < ny)
            def _(d=d, c=c):
                total_copy(d, c).wait_send()


def sums_kernel(scale, chunks, end, under, sums_out, field_out, csum, sum_sem, out_sem):
    J, I = end.shape[:2]
    width = I // chunks

    def out_copy(c):
        here = pl.ds(c * width, width)
        return pltpu.make_async_copy(end.at[:, here], field_out.at[:, here], out_sem.at[c])

    def sum_copy(c):
        here = pl.ds(c * width, width)
        return pltpu.make_async_copy(csum.at[:, here], sums_out.at[:, here], sum_sem.at[c])

    for c in range(chunks):
        out_copy(c).start()
    for c in range(chunks):
        def running(q, carry, c=c):
            i = c * width + q
            value = under[i]
            for j in range(J):
                value = value + end[j, i]
                csum[j, i] = value * scale
            return carry

        lax.fori_loop(0, width, running, 0)
        sum_copy(c).start()
    for c in range(chunks):
        out_copy(c).wait()
        sum_copy(c).wait()


def local(peers, field_now, earlier, speed_square):
    J, I, K, L = field_now.shape
    chunks = CHUNKS if I % CHUNKS == 0 else 1
    ny = peers[0]
    f32 = jnp.float32
    dma = pltpu.SemaphoreType.DMA
    anywhere = pl.BlockSpec(memory_space=pltpu.MemorySpace.HBM)
    shape = jax.ShapeDtypeStruct(field_now.shape, f32)
    slots = max(ny - 1, 1)
    resident = pl.BlockSpec(memory_space=pltpu.VMEM)
    end, under = pl.pallas_call(
        functools.partial(march_kernel, peers, chunks),
        out_shape=(pltpu.VMEM((J, I, K, L), f32), pltpu.VMEM((I, K, L), f32)),
        in_specs=[anywhere] * 3,
        out_specs=(resident, resident),
        scratch_shapes=[
            pltpu.VMEM((2, J + 2, I + 2, K, L), f32),
            pltpu.VMEM((J, I, K, L), f32),
            pltpu.VMEM((I, K, L), f32),
            pltpu.VMEM((slots, I, K, L), f32),
            pltpu.VMEM((STEPS, 2, J, I, L), f32),
            pltpu.VMEM((STEPS, 2, J, I, L), f32),
            dma((5,)),
            dma((STEPS, 2, chunks)),
            dma((STEPS, 2, chunks)),
            dma((STEPS, 2, 3)),
            dma((STEPS, 2, 3)),
            dma((STEPS, 2, 3)),
            dma((STEPS, 2, 3)),
            dma((slots, chunks)),
            dma((slots, chunks)),
        ],
        compiler_params=pltpu.CompilerParams(
            collective_id=0, has_side_effects=True, vmem_limit_bytes=55 * 1024 * 1024
        ),
        name="march",
    )(field_now, earlier, speed_square)
    return pl.pallas_call(
        functools.partial(sums_kernel, 1.0 / (J * ny), chunks),
        out_shape=(shape, shape),
        in_specs=[resident] * 2,
        out_specs=(anywhere, anywhere),
        scratch_shapes=[pltpu.VMEM((J, I, K, L), f32), dma((chunks,)), dma((chunks,))],
        compiler_params=pltpu.CompilerParams(vmem_limit_bytes=16 * 1024 * 1024),
        name="sums",
    )(end, under)


def solution(mesh):
    placed = P("py", "px", "pz", None)
    peers = tuple(mesh.shape[a] for a in ("py", "px", "pz"))
    return jax.shard_map(
        functools.partial(local, peers),
        mesh=mesh,
        in_specs=(placed,) * 3,
        out_specs=(placed,) * 2,
        check_vma=False,
    )
```

```python
import functools

import jax
import jax.numpy as jnp
from jax import lax
from jax.experimental import pallas as pl
from jax.experimental.pallas import tpu as pltpu
from jax.sharding import PartitionSpec as P

STEPS = 4
CHUNKS = 4
MESH = pl.DeviceIdType.MESH


def march_kernel(
    peers, chunks, field, before, speed, end, under,
    u, cs, total, below, ysend, yrecv,
    load_sem, x_send, x_recv, z_send, z_recv, y_send, y_recv, t_send, t_recv, word,
):
    J, I, K, L = field.shape
    ny, nx, nz = peers
    width = I // chunks
    my, mx, mz = (lax.axis_index(a) for a in ("py", "px", "pz"))
    y_side = ({"py": lax.rem(my + 1, ny)}, {"py": lax.rem(my + ny - 1, ny)})
    x_side = ({"px": lax.rem(mx + 1, nx)}, {"px": lax.rem(mx + nx - 1, nx)})
    z_side = ({"pz": lax.rem(mz + 1, nz)}, {"pz": lax.rem(mz + nz - 1, nz)})
    parts = ((1, J - 2), (0, 1), (J - 1, 1))

    loads = [
        pltpu.make_async_copy(
            field.at[pl.ds(start, size)], u.at[0, pl.ds(start + 1, size), pl.ds(1, I)], load_sem.at[part]
        )
        for part, (start, size) in reversed(tuple(enumerate(parts)))
    ] + [
        pltpu.make_async_copy(before, u.at[1, pl.ds(1, J), pl.ds(1, I)], load_sem.at[3]),
        pltpu.make_async_copy(speed, cs, load_sem.at[4]),
    ]
    barrier = pltpu.get_barrier_semaphore()
    above, under_me = mx < nx - 1, mx > 0

    def greet(to):
        pl.semaphore_signal(barrier, inc=1, device_id=to, device_id_type=MESH)

    for d in range(1, ny):
        greet({"py": lax.rem(my + d, ny)})
    for side in z_side:
        greet(side)

    @pl.when(above)
    def _():
        greet(x_side[0])

    @pl.when(under_me)
    def _():
        greet(x_side[1])

    for load in loads:
        load.start()
    pl.semaphore_wait(barrier, ny - 1 + 2 + jnp.where(above, 1, 0) + jnp.where(under_me, 1, 0))

    def hand_on():
        for way, (comes, goes) in enumerate(((under_me, above), (above, under_me))):
            @pl.when(comes)
            def _(way=way):
                pl.semaphore_wait(word.at[way], 1)

            @pl.when(goes)
            def _(way=way):
                pl.semaphore_signal(word.at[way], inc=1, device_id=x_side[way], device_id_type=MESH)

    def remote(src, dst, send, recv, to):
        return pltpu.make_async_remote_copy(
            src_ref=src, dst_ref=dst, send_sem=send, recv_sem=recv, device_id=to, device_id_type=MESH
        )

    def j_copy(t, side, c):
        row, rim = ((J - 1, 0), (0, J + 1))[side]
        there = pl.ds(1 + c * width, width)
        return remote(u.at[t % 2, row + 1, there], u.at[t % 2, rim, there], x_send.at[t, side, c], x_recv.at[t, side, c], y_side[side])

    def i_copy(t, side, part):
        plane, rim = ((I - 1, 0), (0, I + 1))[side]
        start, size = parts[part]
        rows = pl.ds(start + 1, size)
        src = field.at[pl.ds(start, size), plane] if t == 0 else u.at[t % 2, rows, plane + 1]
        return remote(src, u.at[t % 2, rows, rim], z_send.at[t, side, part], z_recv.at[t, side, part], x_side[side])

    def k_copy(t, side, part):
        start, size = parts[part]
        rows = pl.ds(start, size)
        return remote(
            ysend.at[t, side, rows], yrecv.at[t, side, rows],
            y_send.at[t, side, part], y_recv.at[t, side, part], z_side[side],
        )

    def pack(t, j, i, value):
        ysend[t, 0, j, pl.ds(i, 1), :] = value[K - 1:K]
        ysend[t, 1, j, pl.ds(i, 1), :] = value[0:1]

    for side in (0, 1):
        loads[side].wait()
    for c in range(chunks):
        for side in (0, 1):
            j_copy(0, side, c).start()
    hand_on()
    for part in range(3):
        for side in (0, 1):
            i_copy(0, side, part).start()

    loads[2].wait()

    def pack_row(j, carry):
        for i in range(I):
            ysend[0, 0, j, i:i + 1, :] = u[0, j + 1, i + 1, K - 1:K, :]
            ysend[0, 1, j, i:i + 1, :] = u[0, j + 1, i + 1, 0:1, :]
        return carry

    lax.fori_loop(0, J, pack_row, 0)
    for part in range(3):
        for side in (0, 1):
            k_copy(0, side, part).start()
    loads[3].wait()
    loads[4].wait()

    k_index = lax.broadcasted_iota(jnp.int32, (K, L), 0)

    def column(t, j, i):
        now, other = t % 2, (t + 1) % 2
        middle = u[now, j + 1, i + 1]
        low = jnp.where(k_index == 0, yrecv[t, 0, j, pl.ds(i, 1), :], pltpu.roll(middle, 1, 0))
        high = jnp.where(k_index == K - 1, yrecv[t, 1, j, pl.ds(i, 1), :], pltpu.roll(middle, K - 1, 0))
        spread = (
            u[now, j, i + 1] + u[now, j + 2, i + 1] + u[now, j + 1, i] + u[now, j + 1, i + 2]
            + low + high - 6.0 * middle
        )
        later = 2.0 * middle - u[other, j + 1, i + 1] + cs[j, i] * spread
        if t + 1 < STEPS:
            u[other, j + 1, i + 1] = later
            pack(t + 1, j, i, later)
        else:
            end[j, i] = later

    def total_copy(d, c):
        here = pl.ds(c * width, width)
        return remote(
            total.at[here], below.at[d - 1, here], t_send.at[d - 1, c], t_recv.at[d - 1, c],
            {"py": lax.rem(my + d, ny)},
        )

    for t in range(STEPS):
        last = t + 1 == STEPS
        for side in (0, 1):
            i_copy(t, side, 0).wait_recv()
            k_copy(t, side, 0).wait_recv()
            if t > 0:
                i_copy(t - 1, side, 0).wait_send()

        def inner(q, carry, t=t):
            j = 1 + q // (I // 2)
            i = lax.rem(q, I // 2) * 2
            column(t, j, i)
            column(t, j, i + 1)
            return carry

        lax.fori_loop(0, (J - 2) * (I // 2), inner, 0)
        if not last:
            for side in (0, 1):
                i_copy(t + 1, side, 0).start()
                k_copy(t + 1, side, 0).start()

        for side in (0, 1):
            for part in (1, 2):
                i_copy(t, side, part).wait_recv()
                k_copy(t, side, part).wait_recv()
                if t > 0:
                    i_copy(t - 1, side, part).wait_send()
        for c in range(chunks):
            for side in (0, 1):
                j_copy(t, side, c).wait_recv()
                if t > 0:
                    j_copy(t - 1, side, c).wait_send()

            def outer(q, carry, t=t, c=c):
                i = c * width + q
                column(t, 0, i)
                column(t, J - 1, i)
                return carry

            lax.fori_loop(0, width, outer, 0)
            if not last:
                for side in (0, 1):
                    j_copy(t + 1, side, c).start()
            else:
                def add_up(q, carry, c=c):
                    i = c * width + q
                    value = end[0, i]
                    for j in range(1, J):
                        value = value + end[j, i]
                    total[i] = value
                    return carry

                lax.fori_loop(0, width, add_up, 0)
                for d in range(1, ny):
                    @pl.when(my + d < ny)
                    def _(d=d, c=c):
                        total_copy(d, c).start()
        if not last:
            for part in (1, 2):
                for side in (0, 1):
                    i_copy(t + 1, side, part).start()
                    k_copy(t + 1, side, part).start()

    for c in range(chunks):
        here = pl.ds(c * width, width)
        under[here] = jnp.zeros((width, K, L), jnp.float32)
        for d in range(1, ny):
            @pl.when(my >= d)
            def _(d=d, c=c, here=here):
                total_copy(d, c).wait_recv()
                under[here] = under[here] + below[d - 1, here]

    for side in (0, 1):
        for c in range(chunks):
            j_copy(STEPS - 1, side, c).wait_send()
        for part in range(3):
            i_copy(STEPS - 1, side, part).wait_send()
            for t in range(STEPS):
                k_copy(t, side, part).wait_send()
    for c in range(chunks):
        for d in range(1, ny):
            @pl.when(my + d < ny)
            def _(d=d, c=c):
                total_copy(d, c).wait_send()


def sums_kernel(scale, chunks, end, under, sums_out, field_out, csum, sum_sem, out_sem):
    J, I = end.shape[:2]
    width = I // chunks

    def out_copy(c):
        here = pl.ds(c * width, width)
        return pltpu.make_async_copy(end.at[:, here], field_out.at[:, here], out_sem.at[c])

    def sum_copy(c):
        here = pl.ds(c * width, width)
        return pltpu.make_async_copy(csum.at[:, here], sums_out.at[:, here], sum_sem.at[c])

    for c in range(chunks):
        out_copy(c).start()
    for c in range(chunks):
        def running(q, carry, c=c):
            i = c * width + q
            value = under[i]
            for j in range(J):
                value = value + end[j, i]
                csum[j, i] = value * scale
            return carry

        lax.fori_loop(0, width, running, 0)
        sum_copy(c).start()
    for c in range(chunks):
        out_copy(c).wait()
        sum_copy(c).wait()


def local(peers, field_now, earlier, speed_square):
    J, I, K, L = field_now.shape
    chunks = CHUNKS if I % CHUNKS == 0 else 1
    ny = peers[0]
    f32 = jnp.float32
    dma = pltpu.SemaphoreType.DMA
    anywhere = pl.BlockSpec(memory_space=pltpu.MemorySpace.HBM)
    shape = jax.ShapeDtypeStruct(field_now.shape, f32)
    slots = max(ny - 1, 1)
    resident = pl.BlockSpec(memory_space=pltpu.VMEM)
    end, under = pl.pallas_call(
        functools.partial(march_kernel, peers, chunks),
        out_shape=(pltpu.VMEM((J, I, K, L), f32), pltpu.VMEM((I, K, L), f32)),
        in_specs=[anywhere] * 3,
        out_specs=(resident, resident),
        scratch_shapes=[
            pltpu.VMEM((2, J + 2, I + 2, K, L), f32),
            pltpu.VMEM((J, I, K, L), f32),
            pltpu.VMEM((I, K, L), f32),
            pltpu.VMEM((slots, I, K, L), f32),
            pltpu.VMEM((STEPS, 2, J, I, L), f32),
            pltpu.VMEM((STEPS, 2, J, I, L), f32),
            dma((5,)),
            dma((STEPS, 2, chunks)),
            dma((STEPS, 2, chunks)),
            dma((STEPS, 2, 3)),
            dma((STEPS, 2, 3)),
            dma((STEPS, 2, 3)),
            dma((STEPS, 2, 3)),
            dma((slots, chunks)),
            dma((slots, chunks)),
            pltpu.SemaphoreType.REGULAR((2,)),
        ],
        compiler_params=pltpu.CompilerParams(
            collective_id=0, has_side_effects=True, vmem_limit_bytes=55 * 1024 * 1024
        ),
        name="march",
    )(field_now, earlier, speed_square)
    return pl.pallas_call(
        functools.partial(sums_kernel, 1.0 / (J * ny), chunks),
        out_shape=(shape, shape),
        in_specs=[resident] * 2,
        out_specs=(anywhere, anywhere),
        scratch_shapes=[pltpu.VMEM((J, I, K, L), f32), dma((chunks,)), dma((chunks,))],
        compiler_params=pltpu.CompilerParams(vmem_limit_bytes=16 * 1024 * 1024),
        name="sums",
    )(end, under)


def solution(mesh):
    placed = P("py", "px", "pz", None)
    peers = tuple(mesh.shape[a] for a in ("py", "px", "pz"))
    return jax.shard_map(
        functools.partial(local, peers),
        mesh=mesh,
        in_specs=(placed,) * 3,
        out_specs=(placed,) * 2,
        check_vma=False,
    )
```

```python
import functools

import jax
import jax.numpy as jnp
from jax import lax
from jax.experimental import pallas as pl
from jax.experimental.pallas import tpu as pltpu
from jax.sharding import PartitionSpec as P

STEPS = 4
CHUNKS = 4
MESH = pl.DeviceIdType.MESH


def march_kernel(
    peers, chunks, field, before, speed, end, under,
    u, cs, total, below, ysend, yrecv,
    load_sem, x_send, x_recv, z_send, z_recv, y_send, y_recv, t_send, t_recv, word,
):
    J, I, K, L = field.shape
    ny, nx, nz = peers
    width = I // chunks
    my, mx, mz = (lax.axis_index(a) for a in ("py", "px", "pz"))
    y_side = ({"py": lax.rem(my + 1, ny)}, {"py": lax.rem(my + ny - 1, ny)})
    x_side = ({"px": lax.rem(mx + 1, nx)}, {"px": lax.rem(mx + nx - 1, nx)})
    z_side = ({"pz": lax.rem(mz + 1, nz)}, {"pz": lax.rem(mz + nz - 1, nz)})
    parts = ((1, J - 2), (0, 1), (J - 1, 1))

    loads = [
        pltpu.make_async_copy(
            field.at[pl.ds(start, size)], u.at[0, pl.ds(start + 1, size), pl.ds(1, I)], load_sem.at[part]
        )
        for part, (start, size) in reversed(tuple(enumerate(parts)))
    ] + [
        pltpu.make_async_copy(before, u.at[1, pl.ds(1, J), pl.ds(1, I)], load_sem.at[3]),
        pltpu.make_async_copy(speed, cs, load_sem.at[4]),
    ]
    barrier = pltpu.get_barrier_semaphore()
    above, under_me = mx < nx - 1, mx > 0

    def greet(to):
        pl.semaphore_signal(barrier, inc=1, device_id=to, device_id_type=MESH)

    for d in range(1, ny):
        greet({"py": lax.rem(my + d, ny)})
    for side in z_side:
        greet(side)

    @pl.when(above)
    def _():
        greet(x_side[0])

    @pl.when(under_me)
    def _():
        greet(x_side[1])

    for load in loads[:2]:
        load.start()
    pl.semaphore_wait(barrier, ny - 1 + 2 + jnp.where(above, 1, 0) + jnp.where(under_me, 1, 0))

    def hand_on():
        for way, (comes, goes) in enumerate(((under_me, above), (above, under_me))):
            @pl.when(comes)
            def _(way=way):
                pl.semaphore_wait(word.at[way], 1)

            @pl.when(goes)
            def _(way=way):
                pl.semaphore_signal(word.at[way], inc=1, device_id=x_side[way], device_id_type=MESH)

    def remote(src, dst, send, recv, to):
        return pltpu.make_async_remote_copy(
            src_ref=src, dst_ref=dst, send_sem=send, recv_sem=recv, device_id=to, device_id_type=MESH
        )

    def j_copy(t, side, c):
        row, rim = ((J - 1, 0), (0, J + 1))[side]
        there = pl.ds(1 + c * width, width)
        return remote(u.at[t % 2, row + 1, there], u.at[t % 2, rim, there], x_send.at[t, side, c], x_recv.at[t, side, c], y_side[side])

    def i_copy(t, side, part):
        plane, rim = ((I - 1, 0), (0, I + 1))[side]
        start, size = parts[part]
        rows = pl.ds(start + 1, size)
        src = field.at[pl.ds(start, size), plane] if t == 0 else u.at[t % 2, rows, plane + 1]
        return remote(src, u.at[t % 2, rows, rim], z_send.at[t, side, part], z_recv.at[t, side, part], x_side[side])

    def k_copy(t, side, part):
        start, size = parts[part]
        rows = pl.ds(start, size)
        return remote(
            ysend.at[t, side, rows], yrecv.at[t, side, rows],
            y_send.at[t, side, part], y_recv.at[t, side, part], z_side[side],
        )

    def pack(t, j, i, value):
        ysend[t, 0, j, pl.ds(i, 1), :] = value[K - 1:K]
        ysend[t, 1, j, pl.ds(i, 1), :] = value[0:1]

    for side in (0, 1):
        loads[side].wait()
    for c in range(chunks):
        for side in (0, 1):
            j_copy(0, side, c).start()
    for load in loads[2:]:
        load.start()
    hand_on()
    for part in range(3):
        for side in (0, 1):
            i_copy(0, side, part).start()

    loads[2].wait()

    def pack_row(j, carry):
        for i in range(I):
            ysend[0, 0, j, i:i + 1, :] = u[0, j + 1, i + 1, K - 1:K, :]
            ysend[0, 1, j, i:i + 1, :] = u[0, j + 1, i + 1, 0:1, :]
        return carry

    lax.fori_loop(0, J, pack_row, 0)
    for part in range(3):
        for side in (0, 1):
            k_copy(0, side, part).start()
    loads[3].wait()
    loads[4].wait()

    k_index = lax.broadcasted_iota(jnp.int32, (K, L), 0)

    def column(t, j, i):
        now, other = t % 2, (t + 1) % 2
        middle = u[now, j + 1, i + 1]
        low = jnp.where(k_index == 0, yrecv[t, 0, j, pl.ds(i, 1), :], pltpu.roll(middle, 1, 0))
        high = jnp.where(k_index == K - 1, yrecv[t, 1, j, pl.ds(i, 1), :], pltpu.roll(middle, K - 1, 0))
        spread = (
            u[now, j, i + 1] + u[now, j + 2, i + 1] + u[now, j + 1, i] + u[now, j + 1, i + 2]
            + low + high - 6.0 * middle
        )
        later = 2.0 * middle - u[other, j + 1, i + 1] + cs[j, i] * spread
        if t + 1 < STEPS:
            u[other, j + 1, i + 1] = later
            pack(t + 1, j, i, later)
        else:
            end[j, i] = later

    def total_copy(d, c):
        here = pl.ds(c * width, width)
        return remote(
            total.at[here], below.at[d - 1, here], t_send.at[d - 1, c], t_recv.at[d - 1, c],
            {"py": lax.rem(my + d, ny)},
        )

    for t in range(STEPS):
        last = t + 1 == STEPS
        for side in (0, 1):
            i_copy(t, side, 0).wait_recv()
            k_copy(t, side, 0).wait_recv()
            if t > 0:
                i_copy(t - 1, side, 0).wait_send()

        def inner(q, carry, t=t):
            j = 1 + q // (I // 2)
            i = lax.rem(q, I // 2) * 2
            column(t, j, i)
            column(t, j, i + 1)
            return carry

        lax.fori_loop(0, (J - 2) * (I // 2), inner, 0)
        if not last:
            for side in (0, 1):
                i_copy(t + 1, side, 0).start()
                k_copy(t + 1, side, 0).start()

        for side in (0, 1):
            for part in (1, 2):
                i_copy(t, side, part).wait_recv()
                k_copy(t, side, part).wait_recv()
                if t > 0:
                    i_copy(t - 1, side, part).wait_send()
        for c in range(chunks):
            for side in (0, 1):
                j_copy(t, side, c).wait_recv()
                if t > 0:
                    j_copy(t - 1, side, c).wait_send()

            def outer(q, carry, t=t, c=c):
                i = c * width + q
                column(t, 0, i)
                column(t, J - 1, i)
                return carry

            lax.fori_loop(0, width, outer, 0)
            if not last:
                for side in (0, 1):
                    j_copy(t + 1, side, c).start()
            else:
                def add_up(q, carry, c=c):
                    i = c * width + q
                    value = end[0, i]
                    for j in range(1, J):
                        value = value + end[j, i]
                    total[i] = value
                    return carry

                lax.fori_loop(0, width, add_up, 0)
                for d in range(1, ny):
                    @pl.when(my + d < ny)
                    def _(d=d, c=c):
                        total_copy(d, c).start()
        if not last:
            for part in (1, 2):
                for side in (0, 1):
                    i_copy(t + 1, side, part).start()
                    k_copy(t + 1, side, part).start()

    for c in range(chunks):
        here = pl.ds(c * width, width)
        under[here] = jnp.zeros((width, K, L), jnp.float32)
        for d in range(1, ny):
            @pl.when(my >= d)
            def _(d=d, c=c, here=here):
                total_copy(d, c).wait_recv()
                under[here] = under[here] + below[d - 1, here]

    for side in (0, 1):
        for c in range(chunks):
            j_copy(STEPS - 1, side, c).wait_send()
        for part in range(3):
            i_copy(STEPS - 1, side, part).wait_send()
            for t in range(STEPS):
                k_copy(t, side, part).wait_send()
    for c in range(chunks):
        for d in range(1, ny):
            @pl.when(my + d < ny)
            def _(d=d, c=c):
                total_copy(d, c).wait_send()


def sums_kernel(scale, chunks, end, under, sums_out, field_out, csum, sum_sem, out_sem):
    J, I = end.shape[:2]
    width = I // chunks

    def out_copy(c):
        here = pl.ds(c * width, width)
        return pltpu.make_async_copy(end.at[:, here], field_out.at[:, here], out_sem.at[c])

    def sum_copy(c):
        here = pl.ds(c * width, width)
        return pltpu.make_async_copy(csum.at[:, here], sums_out.at[:, here], sum_sem.at[c])

    for c in range(chunks):
        out_copy(c).start()
    for c in range(chunks):
        def running(q, carry, c=c):
            i = c * width + q
            value = under[i]
            for j in range(J):
                value = value + end[j, i]
                csum[j, i] = value * scale
            return carry

        lax.fori_loop(0, width, running, 0)
        sum_copy(c).start()
    for c in range(chunks):
        out_copy(c).wait()
        sum_copy(c).wait()


def local(peers, field_now, earlier, speed_square):
    J, I, K, L = field_now.shape
    chunks = CHUNKS if I % CHUNKS == 0 else 1
    ny = peers[0]
    f32 = jnp.float32
    dma = pltpu.SemaphoreType.DMA
    anywhere = pl.BlockSpec(memory_space=pltpu.MemorySpace.HBM)
    shape = jax.ShapeDtypeStruct(field_now.shape, f32)
    slots = max(ny - 1, 1)
    resident = pl.BlockSpec(memory_space=pltpu.VMEM)
    end, under = pl.pallas_call(
        functools.partial(march_kernel, peers, chunks),
        out_shape=(pltpu.VMEM((J, I, K, L), f32), pltpu.VMEM((I, K, L), f32)),
        in_specs=[anywhere] * 3,
        out_specs=(resident, resident),
        scratch_shapes=[
            pltpu.VMEM((2, J + 2, I + 2, K, L), f32),
            pltpu.VMEM((J, I, K, L), f32),
            pltpu.VMEM((I, K, L), f32),
            pltpu.VMEM((slots, I, K, L), f32),
            pltpu.VMEM((STEPS, 2, J, I, L), f32),
            pltpu.VMEM((STEPS, 2, J, I, L), f32),
            dma((5,)),
            dma((STEPS, 2, chunks)),
            dma((STEPS, 2, chunks)),
            dma((STEPS, 2, 3)),
            dma((STEPS, 2, 3)),
            dma((STEPS, 2, 3)),
            dma((STEPS, 2, 3)),
            dma((slots, chunks)),
            dma((slots, chunks)),
            pltpu.SemaphoreType.REGULAR((2,)),
        ],
        compiler_params=pltpu.CompilerParams(
            collective_id=0, has_side_effects=True, vmem_limit_bytes=55 * 1024 * 1024
        ),
        name="march",
    )(field_now, earlier, speed_square)
    return pl.pallas_call(
        functools.partial(sums_kernel, 1.0 / (J * ny), chunks),
        out_shape=(shape, shape),
        in_specs=[resident] * 2,
        out_specs=(anywhere, anywhere),
        scratch_shapes=[pltpu.VMEM((J, I, K, L), f32), dma((chunks,)), dma((chunks,))],
        compiler_params=pltpu.CompilerParams(vmem_limit_bytes=16 * 1024 * 1024),
        name="sums",
    )(end, under)


def solution(mesh):
    placed = P("py", "px", "pz", None)
    peers = tuple(mesh.shape[a] for a in ("py", "px", "pz"))
    return jax.shard_map(
        functools.partial(local, peers),
        mesh=mesh,
        in_specs=(placed,) * 3,
        out_specs=(placed,) * 2,
        check_vma=False,
    )
```
